32 devices in a mesh: dp: 2 (over core), row: 4 (over y, x), col: 4 (over z).
Axes of the slice: x: 2, y: 2, z: 4, core: 2. Of those that a mesh axis runs over, the one named last changes fastest.
Arguments:
- compressed: float32 [24576, 767], P(('dp', 'row', 'col')), may hold values from -6 to 6
- qkv_weight: bfloat16 [768, 3, 768], P('row', None, 'col'), may hold values from -0.21875 to 0.21875
- qkv_bias: bfloat16 [2, 768], P(None, 'col'), may hold values from -3 to 3
- proj_weight: bfloat16 [768, 768], P('row', 'col'), may hold values from -3 to 3
- proj_bias: bfloat16 [768], replicated, may hold values from -1.75 to 1.75
- attn_gain: bfloat16 [768], replicated, may hold values from 0.5 to 1.5
- mlp_gain: bfloat16 [768], replicated, may hold values from 0.5 to 1.5
- up_weight: bfloat16 [768, 3072], P('row', 'col'), may hold values from -0.21875 to 0.21875
- up_bias: bfloat16 [3072], P('col'), may hold values from -3 to 3
- down_weight: bfloat16 [768, 3072], P('row', 'col'), may hold values from -0.109375 to 0.109375
- down_bias: bfloat16 [768], replicated, may hold values from -1.75 to 1.75
- dealing: int32 [8, 3072], P(('dp', 'row')), may hold values from 0 to 3071, each once within a row
- seq_lengths: int32 [8, 3], P(('dp', 'row')), may hold values from 1 to 2048, 3072 in all within a row
- pad_offsets: int32 [8, 3], P(('dp', 'row')), may hold values from 0 to 255
- cotangent: float32 [24576, 767], P(('dp', 'row', 'col')), may hold values from -6 to 6
Outputs:
- layer_out: float32 [24576, 767], P(('dp', 'row', 'col'))
- input_grad: float32 [24576, 767], P(('dp', 'row', 'col'))
- qkv_weight_grad: float32 [768, 3, 768], P('row', None, 'col')
- qkv_bias_grad: float32 [2, 768], P(None, 'col')
- proj_weight_grad: float32 [768, 768], P('row', 'col')
- proj_bias_grad: float32 [768], replicated
- attn_gain_grad: float32 [768], replicated
- mlp_gain_grad: float32 [768], replicated
- up_weight_grad: float32 [768, 3072], P('row', 'col')
- up_bias_grad: float32 [3072], P('col')
- down_weight_grad: float32 [768, 3072], P('row', 'col')
- down_bias_grad: float32 [768], replicated
The draws below stay inside these ranges and needn't reach their ends.
Inputs may be any that keep to these rules, and one draw needn't show every extreme that they name: `dealing`: each row is an ordering of 0 to 3071. `seq_lengths`: each row sums to 3072; the longest sequence of every bin has exactly 2048 tokens.
All inputs are finite; a program needn't handle non-finite values.
Results may differ from the reference program's by a relative error of at most 0.0072.
Values may be sent and summed in bfloat16 or wider, within the bound.
A program may use at most 192 MiB of HBM per device.

```python
import math
import jax
import jax.numpy as jnp
import numpy as np
from jax import lax

D = 768
H = 12
HD = 64
FF = 3072
BIN_TOK = 3072
SEQ_MAX = 2048
QBLK = 512
PAD_MOST = 256
SEQB = 3
DC = 767
BINS = 8
TOKENS = 24576


def touch_ends(array, own_key, least, top_value):
    place = [jax.random.randint(jax.random.fold_in(own_key, axis), (), 0, length) for axis, length in enumerate(array.shape)]
    longest = array.shape.index(max(array.shape))
    beside = place[:longest] + [(place[longest] + 1) % array.shape[longest]] + place[longest + 1:]
    return array.at[tuple(place)].set(least).at[tuple(beside)].set(top_value)


def level_of(stream_key, dims, cuts, low, high):
    def one(dim, blocks):
        steps = jax.random.uniform(jax.random.fold_in(jax.random.fold_in(stream_key, 6), dim), (blocks,), jnp.float32, low / len(cuts), high / len(cuts))
        return jnp.repeat(jnp.exp(steps), dims[dim] // blocks).reshape((-1,) + (1,) * (len(dims) - dim - 1))

    level = one(*cuts[0])
    for cut in cuts[1:]:
        level = level * one(*cut)
    return level


def profile(amount, total, most, slope):
    weights = [(1 << 20) // math.isqrt(rank ** slope) + 1 for rank in range(2, amount + 1)]
    spare, given = total - most - (amount - 1), [1] * (amount - 1)
    while spare > 0:
        candidates = [i for i in range(amount - 1) if given[i] < most]
        pool, left = sum([weights[i] for i in candidates]), spare
        for i in candidates:
            more = min(most - given[i], max(1, left * weights[i] // pool), spare)
            given[i] = given[i] + more
            spare = spare - more
    return np.array([most] + given)


def uneven(stream_key, count, total, bound, slope):
    if count == 2:
        one = jax.random.randint(stream_key, (), max(1, total - bound), min(bound, total - 1) + 1)
        return jnp.stack([one, total - one])
    lengths = jnp.asarray(profile(count, total, bound, slope), jnp.int32)
    couples = (count - 1) // 2
    source_of, receiver = lengths[1:1 + 2 * couples:2], lengths[2:2 + 2 * couples:2]
    slack = jnp.minimum(source_of - 1, bound - receiver)
    passed = jax.random.randint(jax.random.fold_in(stream_key, 1), (couples,), 0, 1 << 20) % (slack + 1)
    lengths = lengths.at[1:1 + 2 * couples:2].set(source_of - passed).at[2:2 + 2 * couples:2].set(receiver + passed)
    return lengths[jax.random.permutation(jax.random.fold_in(stream_key, 2), count)]


def centred(own_key, dims, width, reach, pieces=(), kind=jnp.bfloat16):
    values = width * jax.random.normal(own_key, dims, jnp.float32)
    if pieces:
        values = values * level_of(own_key, dims, pieces, -0.22, 0.18)
    return jnp.clip(values, -reach, reach).astype(kind)


def setup_inputs(seed: int = 0) -> dict:
    key_of = jax.random.split(jax.random.key(seed), 16)
    compressed = centred(key_of[0], (TOKENS, DC), 1.0, 6.0, ((0, 32),), jnp.float32)
    qkv_weight = centred(key_of[1], (D, 3, D), D ** -0.5, 0.21875, ((0, 4), (2, 4)))
    qkv_bias = centred(key_of[2], (2, D), 0.5, 3.0, ((1, 4),))
    proj_weight = centred(key_of[3], (D, D), 4 ** -0.5, 3.0, ((0, 4), (1, 4)))
    proj_bias = centred(key_of[4], (D,), 0.3, 1.75)
    attn_gain = jnp.clip(1.0 + 0.1 * jax.random.normal(key_of[5], (D,), jnp.float32), 0.5, 1.5).astype(jnp.bfloat16)
    mlp_gain = jnp.clip(1.0 + 0.1 * jax.random.normal(key_of[6], (D,), jnp.float32), 0.5, 1.5).astype(jnp.bfloat16)
    up_weight = centred(key_of[7], (D, FF), D ** -0.5, 0.21875, ((0, 4), (1, 4)))
    up_bias = centred(key_of[8], (FF,), 0.5, 3.0, ((0, 4),))
    down_weight = centred(key_of[9], (D, FF), FF ** -0.5, 0.109375, ((0, 4), (1, 4)))
    down_bias = centred(key_of[10], (D,), 0.3, 1.75)
    dealing = jax.vmap(lambda own: jax.random.permutation(own, BIN_TOK))(jax.random.split(key_of[11], BINS)).reshape((BINS, BIN_TOK)).astype(jnp.int32)
    seq_lengths = jax.vmap(lambda own: uneven(own, SEQB, BIN_TOK, SEQ_MAX, 2))(jax.random.split(key_of[12], BINS)).reshape((BINS, SEQB)).astype(jnp.int32)
    pad_offsets = touch_ends(jax.random.randint(key_of[13], (BINS, SEQB), 0, PAD_MOST), jax.random.fold_in(key_of[13], 1), 0, PAD_MOST - 1).astype(jnp.int32)
    cotangent = centred(key_of[14], (TOKENS, DC), 1.0, 6.0, ((0, 32),), jnp.float32)
    return dict(compressed=compressed, qkv_weight=qkv_weight, qkv_bias=qkv_bias, proj_weight=proj_weight, proj_bias=proj_bias, attn_gain=attn_gain, mlp_gain=mlp_gain, up_weight=up_weight, up_bias=up_bias, down_weight=down_weight, down_bias=down_bias, dealing=dealing, seq_lengths=seq_lengths, pad_offsets=pad_offsets, cotangent=cotangent)


EPS = 1e-05
HIGH = lax.Precision.HIGHEST

@jax.custom_vjp
def low(v):
    return lax.optimization_barrier(v.astype(jnp.bfloat16)).astype(jnp.float32)

@jax.custom_vjp
def low_back(v):
    return v

def low_keep(v):
    return (low(v), None)

def low_pass(kept, grad):
    return (grad,)

def back_keep(v):
    return (v, None)

def back_low(kept, grad):
    return (low(grad),)
low.defvjp(low_keep, low_pass)
low_back.defvjp(back_keep, back_low)

def crms(values, gain_vec):
    return values * lax.rsqrt(lax.optimization_barrier(jnp.mean(values * values, axis=-1, keepdims=True)) + EPS) * gain_vec

def mask_parts(length_row, offset_row, bin_tokens):
    ends = jnp.cumsum(length_row).astype(jnp.int32)
    starts = (ends - length_row).astype(jnp.int32)
    position = jnp.arange(bin_tokens, dtype=jnp.int32)
    segment = lax.optimization_barrier(jnp.sum((position[:, None] >= ends[None, :]).astype(jnp.int32), axis=1)).astype(jnp.int32)
    picks = (segment[:, None] == jnp.arange(length_row.shape[0], dtype=jnp.int32)[None, :]).astype(jnp.int32)
    start_of = lax.optimization_barrier(jnp.sum(picks * starts[None, :], axis=1)).astype(jnp.int32)
    offset_of = lax.optimization_barrier(jnp.sum(picks * offset_row[None, :], axis=1)).astype(jnp.int32)
    return (position, segment, position - start_of >= offset_of)

def bin_forward(rows, order_row, length_row, offset_row, weights):
    qkv_weight, qkv_bias, proj_weight, proj_bias, attn_gain, mlp_gain, up_weight, up_bias, down_weight, down_bias = weights
    scale = HD ** (-0.5)
    decompressed = jnp.concatenate([rows, -lax.optimization_barrier(jnp.sum(rows, axis=1, keepdims=True))], axis=1)
    normed_one = low(crms(decompressed, attn_gain))
    projected = jnp.einsum('td,dje->jte', normed_one, qkv_weight, precision=HIGH)
    queries = low_back(low(projected[0] + qkv_bias[0]))
    keys_all = low_back(low(projected[1]))
    values_all = low_back(low(projected[2] + qkv_bias[1]))
    query_heads = queries[order_row].reshape(BIN_TOK, H, HD)
    key_heads = keys_all[order_row].reshape(BIN_TOK, H, HD)
    value_heads = values_all[order_row].reshape(BIN_TOK, H, HD)
    position, segment, valid = mask_parts(length_row, offset_row, BIN_TOK)

    def attend_block(block_index):
        first_row = block_index * QBLK
        query_block = lax.dynamic_slice_in_dim(query_heads, first_row, QBLK, 0)
        row_pos = lax.dynamic_slice_in_dim(position, first_row, QBLK, 0)
        row_seg = lax.dynamic_slice_in_dim(segment, first_row, QBLK, 0)
        scores = low_back(jnp.einsum('qhd,khd->hqk', query_block, key_heads, precision=HIGH) * scale)
        allowed = (row_seg[:, None] == segment[None, :]) & (position[None, :] <= row_pos[:, None]) & (valid[None, :] | (position[None, :] == row_pos[:, None]))
        scores = jnp.where(allowed[None], scores, -jnp.inf)
        row_max = lax.optimization_barrier(jnp.max(scores, axis=2, keepdims=True))
        weights_exp = jnp.exp(scores - row_max)
        probs = low(weights_exp / lax.optimization_barrier(jnp.sum(weights_exp, axis=2, keepdims=True)))
        return jnp.einsum('hqk,khd->qhd', probs, value_heads, precision=HIGH)
    attended = lax.map(jax.checkpoint(attend_block), jnp.arange(BIN_TOK // QBLK, dtype=jnp.int32))
    attended = attended.reshape(BIN_TOK, D)
    attended_given = low_back(low(jnp.zeros_like(attended).at[order_row].set(attended)))
    branch_one = low_back(jnp.einsum('ti,oi->to', attended_given, proj_weight, precision=HIGH) + proj_bias)
    residual_two = decompressed + branch_one - lax.optimization_barrier(jnp.mean(branch_one, axis=1, keepdims=True))
    normed_two = low(crms(residual_two, mlp_gain))
    pre_act = low_back(jnp.dot(normed_two, up_weight, precision=HIGH) + up_bias)
    hidden = low(jax.nn.gelu(pre_act, approximate=True))
    branch_two = low_back(jnp.einsum('tf,of->to', hidden, down_weight, precision=HIGH) + down_bias)
    residual_three = residual_two + branch_two - lax.optimization_barrier(jnp.mean(branch_two, axis=1, keepdims=True))
    return residual_three[:, :D - 1]

def reference(compressed, qkv_weight, qkv_bias, proj_weight, proj_bias, attn_gain, mlp_gain, up_weight, up_bias, down_weight, down_bias, dealing, seq_lengths, pad_offsets, cotangent):
    params = (qkv_weight.astype(jnp.float32), qkv_bias.astype(jnp.float32), proj_weight.astype(jnp.float32), proj_bias.astype(jnp.float32), attn_gain.astype(jnp.float32), mlp_gain.astype(jnp.float32), up_weight.astype(jnp.float32), up_bias.astype(jnp.float32), down_weight.astype(jnp.float32), down_bias.astype(jnp.float32))

    def whole(flat, weights):
        binned = flat.reshape(BINS, BIN_TOK, D - 1)

        def one_bin(packed):
            rows, order_row, length_row, offset_row = packed
            return bin_forward(rows, order_row, length_row, offset_row, weights)
        return lax.map(one_bin, (binned, dealing, seq_lengths, pad_offsets)).reshape(TOKENS, D - 1)
    layer_out, pullback = jax.vjp(whole, compressed.astype(jnp.float32), params)
    input_grad, grads = pullback(cotangent.astype(jnp.float32))
    return (layer_out, input_grad, grads[0], grads[1], grads[2], grads[3], grads[4], grads[5], grads[6], grads[7], grads[8], grads[9])
```

```python
import functools

import jax
import jax.numpy as jnp
from jax import lax
from jax.experimental import pallas as pl
from jax.experimental.pallas import tpu as pltpu
from jax.sharding import PartitionSpec as P

HD = 64
EPS = 1e-05
NEG = -1e30
SCALE = HD ** (-0.5)
ALL = ("dp", "row", "col")
BF = jnp.bfloat16
F32 = jnp.float32
NN = (((1,), (0,)), ((), ()))
NT = (((1,), (1,)), ((), ()))


def mm(a, b, dims):
    return lax.dot_general(a, b, dims, preferred_element_type=F32)


def first_visible(length_row, offset_row, tokens):
    ends = jnp.cumsum(length_row)
    starts = ends - length_row
    position = jnp.arange(tokens, dtype=jnp.int32)
    segment = jnp.sum((position[:, None] >= ends[None, :]).astype(jnp.int32), axis=1)
    picks = (segment[:, None] == jnp.arange(length_row.shape[0], dtype=jnp.int32)[None, :]).astype(
        jnp.int32
    )
    first_real = jnp.sum(picks * (starts + offset_row)[None, :], axis=1)
    return jnp.where(position >= first_real, first_real, position)


def forward_kernel(heads, bk, first_ref, q_ref, k_ref, vt_ref, lo_ref, ot_ref, lse_ref):
    block = pl.program_id(0)
    bq = q_ref.shape[0]
    q0 = block * bq
    lo = lo_ref[...]
    queries = [q_ref[:, h * HD : (h + 1) * HD] for h in range(heads)]
    key_pos = lax.broadcasted_iota(jnp.int32, (bk, bq), 0)
    query_pos = q0 + lax.broadcasted_iota(jnp.int32, (bk, bq), 1)
    last = (q0 + bq - 1) // bk

    def step(i, carry):
        k0 = pl.multiple_of((last - i) * bk, bk)
        t = k0 + key_pos
        seen = (t >= lo) & (t <= query_pos)
        keys = k_ref[pl.ds(k0, bk), :]
        values = vt_ref[:, pl.ds(k0, bk)]
        out = []
        for h in range(heads):
            top, total, acc = carry[h]
            scores = mm(keys[:, h * HD : (h + 1) * HD], queries[h], NT)
            scores = jnp.where(seen, scores, NEG)
            top_new = jnp.maximum(top, jnp.max(scores, axis=0, keepdims=True))
            weights = jnp.exp(scores - top_new)
            fade = jnp.exp(top - top_new)
            total = total * fade + jnp.sum(weights, axis=0, keepdims=True)
            acc = acc * fade + mm(values[h * HD : (h + 1) * HD, :], weights.astype(BF), NN)
            out.append((top_new, total, acc))
        return tuple(out)

    start = tuple(
        (jnp.full((1, bq), NEG, F32), jnp.zeros((1, bq), F32), jnp.zeros((HD, bq), F32))
        for _ in range(heads)
    )
    result = lax.fori_loop(0, last - first_ref[block] + 1, step, start)
    for h in range(heads):
        top, total, acc = result[h]
        ot_ref[h * HD : (h + 1) * HD, :] = acc / total
        lse_ref[h : h + 1, :] = top + jnp.log(total)


def attend(q, k, vt, lo, bq=512, bk=512):
    n, w = q.shape
    heads = w // HD
    return pl.pallas_call(
        functools.partial(forward_kernel, heads, bk),
        out_shape=(jax.ShapeDtypeStruct((w, n), F32), jax.ShapeDtypeStruct((8, n), F32)),
        grid_spec=pltpu.PrefetchScalarGridSpec(
            num_scalar_prefetch=1,
            grid=(n // bq,),
            in_specs=[
                pl.BlockSpec((bq, w), lambda i, s: (i, 0)),
                pl.BlockSpec((n, w), lambda i, s: (0, 0)),
                pl.BlockSpec((w, n), lambda i, s: (0, 0)),
                pl.BlockSpec((1, bq), lambda i, s: (0, i)),
            ],
            out_specs=[
                pl.BlockSpec((w, bq), lambda i, s: (0, i)),
                pl.BlockSpec((8, bq), lambda i, s: (0, i)),
            ],
        ),
        cost_estimate=pl.CostEstimate(flops=10**10, bytes_accessed=10**7, transcendentals=10**7),
        name="attend",
    )(lo[::bq] // bk, q, k, vt, lo[None])


def backward_kernel(
    heads, bq, last_ref, k_ref, v_ref, kt_ref, q_ref, go_ref, lse_ref, dot_ref, lo_ref, out_ref, dq_ref
):
    block = pl.program_id(0)
    bk = k_ref.shape[0]
    w = heads * HD
    k0 = pl.multiple_of(block * bk, bk)

    @pl.when(block == 0)
    def _():
        dq_ref[...] = jnp.zeros_like(dq_ref)

    keys = [k_ref[:, h * HD : (h + 1) * HD] for h in range(heads)]
    values = [v_ref[:, h * HD : (h + 1) * HD] for h in range(heads)]
    keys_t = [kt_ref[h * HD : (h + 1) * HD, :] for h in range(heads)]
    t = k0 + lax.broadcasted_iota(jnp.int32, (bk, bq), 0)
    query_pos = lax.broadcasted_iota(jnp.int32, (bk, bq), 1)
    first = k0 // bq

    def step(i, carry):
        q0 = pl.multiple_of((first + i) * bq, bq)
        lo = lo_ref[:, pl.ds(q0, bq)]
        seen = (t >= lo) & (t <= query_pos + q0)
        q_block = q_ref[pl.ds(q0, bq), :]
        go_block = go_ref[pl.ds(q0, bq), :]
        lse = lse_ref[:, pl.ds(q0, bq)]
        dots = dot_ref[:, pl.ds(q0, bq)]
        out = []
        for h in range(heads):
            dk, dv = carry[h]
            q = q_block[:, h * HD : (h + 1) * HD]
            go = go_block[:, h * HD : (h + 1) * HD]
            scores = jnp.where(seen, mm(keys[h], q, NT) - lse[h : h + 1, :], NEG)
            probs = jnp.exp(scores)
            gp = mm(values[h], go, NT)
            gs = (probs * (gp - dots[h : h + 1, :])).astype(BF)
            dv = dv + mm(probs.astype(BF), go, NN)
            dk = dk + mm(gs, q, NN)
            dq_ref[h * HD : (h + 1) * HD, pl.ds(q0, bq)] += mm(keys_t[h], gs, NN)
            out.append((dk, dv))
        return tuple(out)

    zero = jnp.zeros((bk, HD), F32)
    result = lax.fori_loop(
        0, last_ref[block] - first + 1, step, tuple((zero, zero) for _ in range(heads))
    )
    for h in range(heads):
        out_ref[pl.ds(k0, bk), w + h * HD : w + (h + 1) * HD] = result[h][0].astype(BF)
        out_ref[pl.ds(k0, bk), 2 * w + h * HD : 2 * w + (h + 1) * HD] = result[h][1].astype(BF)

    @pl.when(block == pl.num_programs(0) - 1)
    def _():
        def turn(i, carry):
            at = pl.multiple_of(i * bq, bq)
            out_ref[pl.ds(at, bq), 0:w] = (dq_ref[:, pl.ds(at, bq)].T * SCALE).astype(BF)
            return carry

        lax.fori_loop(0, dq_ref.shape[1] // bq, turn, 0)


def attend_back(q, k, v, go, lse, dots, lo, bq=512, bk=256):
    n, w = q.shape
    heads = w // HD
    ends = (jnp.arange(n // bk, dtype=jnp.int32) + 1) * bk - 1
    last = (jnp.sum((lo[None, :] <= ends[:, None]).astype(jnp.int32), axis=1) - 1) // bq
    whole = lambda r, c: pl.BlockSpec((r, c), lambda i, s: (0, 0))
    return pl.pallas_call(
        functools.partial(backward_kernel, heads, bq),
        out_shape=jax.ShapeDtypeStruct((n, 3 * w), BF),
        grid_spec=pltpu.PrefetchScalarGridSpec(
            num_scalar_prefetch=1,
            grid=(n // bk,),
            in_specs=[
                pl.BlockSpec((bk, w), lambda i, s: (i, 0)),
                pl.BlockSpec((bk, w), lambda i, s: (i, 0)),
                pl.BlockSpec((w, bk), lambda i, s: (0, i)),
                whole(n, w),
                whole(n, w),
                whole(8, n),
                whole(8, n),
                whole(1, n),
            ],
            out_specs=whole(n, 3 * w),
            scratch_shapes=[pltpu.VMEM((w, n), F32)],
        ),
        cost_estimate=pl.CostEstimate(flops=2 * 10**10, bytes_accessed=10**7, transcendentals=10**7),
        name="attend_back",
    )(last, k, v, k.T, q, go, lse, dots, lo[None])


GELU_C = 0.7978845608028654
GELU_A = 0.044715


def middle_kernel(
    sizes,
    o_ref,
    proj_ref,
    x_ref,
    g3_ref,
    vec_ref,
    upb_ref,
    up_ref,
    down_ref,
    lay_ref,
    gx2_ref,
    go_ref,
    sums_ref,
    projg_ref,
    upbg_ref,
    grad_ref,
    x2_ref,
    n2_ref,
    n2t_ref,
    gy2_ref,
    gy2t_ref,
    y2_ref,
    gn2_ref,
    hid_ref,
    gu_ref,
    gy1_ref,
    gy1t_ref,
):
    groups, chunk = sizes
    step = pl.program_id(0)
    tokens, width = x_ref.shape
    gw = width // groups
    chunks = tokens // chunk
    proj_bias, gain, down_bias = vec_ref[0:1, :], vec_ref[1:2, :], vec_ref[2:3, :]

    @pl.when(step == 0)
    def _():
        def rows(i, carry):
            at = pl.ds(pl.multiple_of(i * chunk, chunk), chunk)
            y1 = mm(o_ref[0, at, :], proj_ref[:, 0:gw], NT)
            for g in range(1, groups):
                y1 += mm(o_ref[g, at, :], proj_ref[:, g * gw : (g + 1) * gw], NT)
            y1 += proj_bias
            x2 = x_ref[at, :] + (y1 - jnp.mean(y1, axis=1, keepdims=True))
            x2_ref[at, :] = x2
            r = lax.rsqrt(jnp.mean(x2 * x2, axis=1, keepdims=True) + EPS)
            n2_ref[at, :] = (x2 * r * gain).astype(BF)
            g3 = g3_ref[at, :]
            gy2 = (g3 - jnp.mean(g3, axis=1, keepdims=True)).astype(BF)
            gy2_ref[at, :] = gy2
            return carry + jnp.sum(gy2.astype(F32), axis=0, keepdims=True)

        sums_ref[...] = jnp.zeros_like(sums_ref)
        sums_ref[2:3, :] = lax.fori_loop(0, chunks, rows, jnp.zeros((1, width), F32))
        n2t_ref[...] = n2_ref[...].T
        gy2t_ref[...] = gy2_ref[...].T
        y2_ref[...] = jnp.zeros_like(y2_ref)
        gn2_ref[...] = jnp.zeros_like(gn2_ref)

    up = up_ref[...].reshape(width, up_ref.shape[-1])
    down = down_ref[...].reshape(width, down_ref.shape[-1])
    up_bias = upb_ref[0]

    def hidden(i, carry):
        at = pl.ds(pl.multiple_of(i * chunk, chunk), chunk)
        u = mm(n2_ref[at, :], up, NN) + up_bias
        square = u * u
        th = jnp.tanh(GELU_C * (u + GELU_A * (square * u)))
        hid = (0.5 * u * (1.0 + th)).astype(BF)
        hid_ref[at, :] = hid
        slope = 0.5 * (1.0 + th) + 0.5 * u * (1.0 - th * th) * (
            GELU_C * (1.0 + 3.0 * GELU_A * square)
        )
        gu = (mm(gy2_ref[at, :], down, NN) * slope).astype(BF)
        gu_ref[at, :] = gu
        y2_ref[at, :] += mm(hid, down, NT)
        gn2_ref[at, :] += mm(gu, up, NT)
        return carry + jnp.sum(gu.astype(F32), axis=0, keepdims=True)

    upbg_ref[0] = lax.fori_loop(0, chunks, hidden, jnp.zeros((1, up.shape[1]), F32))
    part = up_ref.shape[-2]
    blocks = width // part
    up_grad = mm(n2t_ref[...], gu_ref[...], NN).astype(BF)
    down_grad = mm(gy2t_ref[...], hid_ref[...], NN).astype(BF)
    grad_ref[0, :, 0, 0:part, :] = up_grad.reshape(blocks, part, up_grad.shape[1])
    grad_ref[0, :, 0, part : 2 * part, :] = down_grad.reshape(blocks, part, up_grad.shape[1])

    @pl.when(step == pl.num_programs(0) - 1)
    def _():
        def rows(i, carry):
            gain_sum, bias_sum = carry
            at = pl.ds(pl.multiple_of(i * chunk, chunk), chunk)
            x2 = x2_ref[at, :]
            y2 = y2_ref[at, :] + down_bias
            lay_ref[at, :] = (x2 + (y2 - jnp.mean(y2, axis=1, keepdims=True)))[:, 0 : width - 1]
            r = lax.rsqrt(jnp.mean(x2 * x2, axis=1, keepdims=True) + EPS)
            gn2 = gn2_ref[at, :]
            gain_sum = gain_sum + jnp.sum(gn2 * (x2 * r), axis=0, keepdims=True)
            gn2 = gn2 * gain
            gx2 = (
                g3_ref[at, :]
                + r * gn2
                - x2 * ((r * r * r) * jnp.mean(gn2 * x2, axis=1, keepdims=True))
            )
            gx2_ref[at, :] = gx2
            gy1 = (gx2 - jnp.mean(gx2, axis=1, keepdims=True)).astype(BF)
            gy1_ref[at, :] = gy1
            go = mm(gy1, proj_ref[...], NN).astype(BF)
            for g in range(groups):
                go_ref[g, at, :] = go[:, g * gw : (g + 1) * gw]
            return gain_sum, bias_sum + jnp.sum(gy1.astype(F32), axis=0, keepdims=True)

        zero = jnp.zeros((1, width), F32)
        gain_sum, bias_sum = lax.fori_loop(0, chunks, rows, (zero, zero))
        sums_ref[0:1, :] = gain_sum
        sums_ref[1:2, :] = bias_sum
        gy1t_ref[...] = gy1_ref[...].T
        for g in range(groups):
            projg_ref[:, g * gw : (g + 1) * gw] = mm(gy1t_ref[...], o_ref[g], NN).astype(BF)


def middle(o, proj, x, g3, vecs, up_bias, gathered, part):
    groups, tokens, gw = o.shape
    width = x.shape[1]
    halves, row_count, col_count, _, block = gathered.shape
    steps = halves * col_count
    chunk = 256
    once = pl.Buffered(buffer_count=1)
    whole = lambda *s: pl.BlockSpec(s, lambda i: (0,) * len(s), pipeline_mode=once)
    keep = lambda *s: pl.BlockSpec(s, lambda i: (0,) * len(s))
    wide = lambda which: pl.BlockSpec(
        (1, row_count, 1, part, block), lambda i: (i % halves, 0, i // halves, which, 0)
    )
    return pl.pallas_call(
        functools.partial(middle_kernel, (groups, chunk)),
        out_shape=(
            jax.ShapeDtypeStruct((tokens, width - 1), F32),
            jax.ShapeDtypeStruct((tokens, width), F32),
            jax.ShapeDtypeStruct((groups, tokens, gw), BF),
            jax.ShapeDtypeStruct((8, width), F32),
            jax.ShapeDtypeStruct((width, width), BF),
            jax.ShapeDtypeStruct((steps, 1, block), F32),
            jax.ShapeDtypeStruct((halves, row_count, col_count, 2 * part, block), BF),
        ),
        grid=(steps,),
        in_specs=[
            whole(groups, tokens, gw),
            whole(width, width),
            whole(tokens, width),
            whole(tokens, width),
            whole(8, width),
            pl.BlockSpec((1, 1, block), lambda i: (i, 0, 0)),
            wide(0),
            wide(1),
        ],
        out_specs=[
            keep(tokens, width - 1),
            keep(tokens, width),
            keep(groups, tokens, gw),
            keep(8, width),
            keep(width, width),
            pl.BlockSpec((1, 1, block), lambda i: (i, 0, 0)),
            pl.BlockSpec(
                (1, row_count, 1, 2 * part, block), lambda i: (i % halves, 0, i // halves, 0, 0)
            ),
        ],
        scratch_shapes=[
            pltpu.VMEM((tokens, width), F32),
            pltpu.VMEM((tokens, width), BF),
            pltpu.VMEM((width, tokens), BF),
            pltpu.VMEM((tokens, width), BF),
            pltpu.VMEM((width, tokens), BF),
            pltpu.VMEM((tokens, width), F32),
            pltpu.VMEM((tokens, width), F32),
            pltpu.VMEM((tokens, block), BF),
            pltpu.VMEM((tokens, block), BF),
            pltpu.VMEM((tokens, width), BF),
            pltpu.VMEM((width, tokens), BF),
        ],
        cost_estimate=pl.CostEstimate(flops=3 * 10**10, bytes_accessed=4 * 10**7, transcendentals=10**7),
        name="middle",
    )(o, proj, x, g3, vecs, up_bias, gathered, gathered)


def local(
    compressed,
    qkv_weight,
    qkv_bias,
    proj_weight,
    proj_bias,
    attn_gain,
    mlp_gain,
    up_weight,
    up_bias,
    down_weight,
    down_bias,
    dealing,
    seq_lengths,
    pad_offsets,
    cotangent,
):
    share = compressed.shape[0]
    dp_count, row_count, col_count = (lax.axis_size(a) for a in ALL)
    half = lax.axis_index("dp")
    tokens = share * col_count
    width = proj_weight.shape[0] * row_count
    part, hidden = up_weight.shape
    w = qkv_weight.shape[2]
    order = dealing[0]
    back = jnp.zeros((tokens,), jnp.int32).at[order].set(jnp.arange(tokens, dtype=jnp.int32))
    lo = first_visible(seq_lengths[0], pad_offsets[0], tokens)

    x = jnp.concatenate([compressed, -jnp.sum(compressed, axis=1, keepdims=True)], axis=1)
    gain1 = attn_gain.astype(F32)
    r1 = lax.rsqrt(jnp.mean(x * x, axis=-1, keepdims=True) + EPS)
    n1 = (x * r1 * gain1).astype(BF)
    g3 = jnp.pad(cotangent, ((0, 0), (0, 1)))

    qkv_rows = lax.all_gather(qkv_weight.reshape(part, 3 * w), "row", axis=0, tiled=True)
    n1_full = lax.all_gather(n1, "col", axis=0, tiled=True)

    block = hidden // dp_count
    cut = lambda a: lax.dynamic_slice_in_dim(a, half * block, block, 1)
    proj_half = lax.dynamic_slice_in_dim(proj_weight, half * (part // dp_count), part // dp_count, 0)
    mine = jnp.concatenate([cut(up_weight), cut(down_weight), proj_half.reshape(-1, block)], axis=0)
    mine, n1_full = lax.optimization_barrier((mine, n1_full))
    gathered = lax.all_gather(mine, ALL, axis=0, tiled=True).reshape(
        dp_count, row_count, col_count, mine.shape[0], block
    )
    proj = (
        gathered[:, :, :, 2 * part :, :]
        .reshape(dp_count, row_count, col_count, part // dp_count, w)
        .transpose(1, 0, 3, 2, 4)
        .reshape(width, width)
    )

    n1_proc = n1_full[order]
    bias = qkv_bias.astype(F32)
    q = (mm(n1_proc, qkv_rows[:, 0:w], NN) + bias[0]).astype(BF) * jnp.asarray(SCALE, BF)
    k = mm(n1_proc, qkv_rows[:, w : 2 * w], NN).astype(BF)
    v = (mm(n1_proc, qkv_rows[:, 2 * w :], NN) + bias[1]).astype(BF)
    ot, lse = attend(q, k, v.T, lo)
    o = ot.T
    o_given = o.astype(BF)[back].reshape(col_count, share, w)
    o_mine = lax.all_to_all(o_given, "col", 0, 0, tiled=True)

    vecs = jnp.pad(
        jnp.stack([proj_bias, mlp_gain, down_bias]).astype(F32), ((0, 5), (0, 0))
    )
    up_bias_all = lax.all_gather(up_bias, "col", axis=0, tiled=True).astype(F32)
    layer_out, gx2, go_mine, sums, proj_grad, up_bias_grad, wide_grad = middle(
        o_mine, proj, x, g3, vecs, up_bias_all.reshape(-1, 1, block), gathered, part
    )

    go_given = lax.all_to_all(go_mine, "col", 0, 0, tiled=True).reshape(tokens, w)
    proj_parts = (
        proj_grad.reshape(row_count, dp_count, part // dp_count, col_count, w)
        .transpose(1, 0, 3, 2, 4)
        .reshape(-1, w)
    )
    wide_sum = lax.psum_scatter(wide_grad.reshape(-1, block), ALL, scatter_dimension=0, tiled=True)
    proj_sum = lax.psum_scatter(proj_parts, ALL, scatter_dimension=0, tiled=True)
    wide_both = lax.all_gather(wide_sum, "dp", axis=0, tiled=False)
    up_total = jnp.concatenate([wide_both[i, 0:part] for i in range(dp_count)], axis=1).astype(F32)
    down_total = jnp.concatenate([wide_both[i, part:] for i in range(dp_count)], axis=1).astype(F32)
    proj_total = lax.all_gather(proj_sum, "dp", axis=0, tiled=True).astype(F32)
    small = jnp.concatenate([sums[0:3].reshape(1, -1), up_bias_grad.reshape(1, -1)], axis=1)
    small_total = jnp.sum(lax.all_gather(small, ALL, axis=0, tiled=True), axis=0)

    go = go_given[order]
    heads = w // HD
    dots = jnp.sum((go.astype(F32) * o).reshape(tokens, heads, HD), axis=2)
    dots = jnp.pad(dots.T, ((0, 8 - heads), (0, 0)))
    gqkv = attend_back(q, k, v, go, lse, dots, lo)

    qkv_grad = lax.dot_general(n1_proc, gqkv, (((0,), (0,)), ((), ())), preferred_element_type=F32)
    gain_part = jnp.sum(qkv_grad * qkv_rows.astype(F32), axis=1) / gain1
    bias_part = jnp.sum(gqkv.astype(F32), axis=0)
    tail = jnp.concatenate([gain_part, bias_part])[None]
    gn1_part = mm(gqkv[back], qkv_rows, NT).astype(BF)
    gn1 = lax.psum_scatter(gn1_part, "col", scatter_dimension=0, tiled=True).astype(F32)
    qkv_parts = (
        qkv_grad.astype(BF)
        .reshape(row_count, dp_count, part // dp_count, 3 * w)
        .transpose(1, 0, 2, 3)
        .reshape(width, 3 * w)
    )
    qkv_sum = lax.psum_scatter(qkv_parts, ("dp", "row"), scatter_dimension=0, tiled=True)
    qkv_total = lax.all_gather(qkv_sum, "dp", axis=0, tiled=True).astype(F32)
    tail_all = lax.all_gather(tail, ALL, axis=0, tiled=True)
    attn_gain_grad = jnp.sum(tail_all[:, 0:width], axis=0)
    col = lax.axis_index("col")
    bias_total = jnp.sum(
        lax.dynamic_index_in_dim(
            tail_all[:, width:].reshape(-1, col_count, 3 * w), col, 1, keepdims=False
        ),
        axis=0,
    )

    scaled = gn1 * gain1
    gx = gx2 + r1 * scaled - x * (r1**3 * jnp.mean(scaled * x, axis=1, keepdims=True))
    input_grad = gx[:, :-1] - gx[:, -1:]
    return (
        layer_out,
        input_grad,
        qkv_total.reshape(part, 3, w),
        jnp.stack([bias_total[0:w], bias_total[2 * w :]]),
        proj_total,
        small_total[width : 2 * width],
        attn_gain_grad,
        small_total[0:width],
        up_total,
        lax.dynamic_slice_in_dim(small_total, 3 * width + col * hidden, hidden, 0),
        down_total,
        small_total[2 * width : 3 * width],
    )


def solution(mesh):
    placed = (
        P(ALL, None),
        P("row", None, "col"),
        P(None, "col"),
        P("row", "col"),
        P(),
        P(),
        P(),
        P("row", "col"),
        P("col"),
        P("row", "col"),
        P(),
        P(("dp", "row"), None),
        P(("dp", "row"), None),
        P(("dp", "row"), None),
        P(ALL, None),
    )
    return jax.shard_map(
        local,
        mesh=mesh,
        in_specs=placed,
        out_specs=(
            P(ALL, None),
            P(ALL, None),
            P("row", None, "col"),
            P(None, "col"),
            P("row", "col"),
            P(),
            P(),
            P(),
            P("row", "col"),
            P("col"),
            P("row", "col"),
            P(),
        ),
        check_vma=False,
    )
```
